256 devices in a mesh: blk: 128 (over y, z, x_hi, core), mp: 2 (over x_lo).
Axes of the slice: x: 4 (x_hi: 2, x_lo: 2; x = x_hi * 2 + x_lo), y: 4, z: 8, core: 2. Of those that a mesh axis runs over, the one named last changes fastest.
Arguments:
- params: bfloat16 [128, 1024, 4096], P('blk', None, 'mp'), may hold values from -0.09375 to 0.09375
- hidden: bfloat16 [128, 384, 4096], P('blk', None, 'mp'), may hold values from -6 to 6
- targets: bfloat16 [128, 384, 1024], P('blk', None, 'mp'), may hold values from -6 to 6
Outputs:
- params_out: bfloat16 [128, 1024, 4096], P('blk', None, 'mp')
- errors: float32 [2], replicated
The draws below stay inside these ranges and needn't reach their ends.
All inputs are finite; a program needn't handle non-finite values.
Results may differ from the reference program's by a relative error of at most 0.0085.
Values may be sent and summed in bfloat16 or wider, within the bound.
A program may use at most 128 MiB of HBM per device.

```python
import jax
import jax.numpy as jnp
from jax import lax

D = 1024
TOK = 384
ITERS = 2
FF_WIN = 4096
REPL = 128


def steps_of(stream_key, dims, shards, least, top_value):
    level = 1.0
    for dim, parts in shards:
        steps = jax.random.uniform(jax.random.fold_in(jax.random.fold_in(stream_key, 6), dim), (parts,), jnp.float32, least / len(shards), top_value / len(shards))
        level = level * jnp.repeat(jnp.exp(steps), dims[dim] // parts).reshape((-1,) + (1,) * (len(dims) - 1 - dim))
    return level


def bell_draw(stream_key, shape, scale, most, cuts=(), kind=jnp.bfloat16):
    gain = steps_of(stream_key, shape, cuts, -0.22, 0.18) if cuts else 1.0
    array = jax.random.normal(stream_key, shape, jnp.float32) * scale * gain
    return jnp.minimum(jnp.maximum(array, -most), most).astype(kind)


def setup_inputs(seed: int = 0) -> dict:
    streams_of = jax.random.split(jax.random.key(seed), 4)
    return {
        "params": bell_draw(streams_of[0], (REPL, D, FF_WIN), FF_WIN ** -0.5, 0.09375, ((0, 128), (2, 2))),
        "hidden": bell_draw(streams_of[1], (REPL, TOK, FF_WIN), 1.0, 6.0, ((0, 128), (2, 2))),
        "targets": bell_draw(streams_of[2], (REPL, TOK, D), 1.0, 6.0, ((0, 128), (2, 2))),
    }


mix_third = 1.0 / 3.0
step_size = 0.1


def gradient(weight, hidden_one, targets_one):
    output = lax.dot_general(hidden_one, weight, (((1,), (1,)), ((), ())), preferred_element_type=jnp.float32)
    resid = (output - targets_one.astype(jnp.float32)).astype(jnp.bfloat16)
    grad = lax.dot_general(resid, hidden_one, (((0,), (0,)), ((), ())), preferred_element_type=jnp.float32)
    return grad / TOK


def one_item(item):
    return gradient(item[0], item[1], item[2])


def pick(stack, index):
    return lax.dynamic_index_in_dim(stack, (index % REPL).astype(jnp.int32), 0, keepdims=False).astype(jnp.float32)


def reference(params, hidden, targets):
    state = params
    older = lax.map(one_item, (params, hidden, targets))
    fresh = older
    track = older.astype(jnp.bfloat16)
    indices = jnp.arange(REPL, dtype=jnp.int32)
    err_list = []
    for step in range(ITERS):
        if step > 0:
            def track_row(index):
                blend = (pick(track, index - 1) + pick(track, index) + pick(track, index + 1)) * mix_third
                return (blend + pick(fresh, index) - pick(older, index)).astype(jnp.bfloat16)
            track = lax.map(track_row, indices)
            older = fresh

        def err_row(index):
            diff = pick(state, index) - pick(state, index + 1)
            return jnp.sum(diff * diff)
        err_list.append(jnp.sum(lax.map(err_row, indices)) / (FF_WIN * REPL))

        def state_row(index):
            blend = (pick(state, index - 1) + pick(state, index) + pick(state, index + 1)) * mix_third
            return (blend - step_size * pick(track, index)).astype(jnp.bfloat16)
        new_state = lax.map(state_row, indices)
        if step < ITERS - 1:
            fresh = lax.map(one_item, (new_state, hidden, targets))
        state = new_state
    return state, jnp.stack(err_list)
```

```python
import functools

import jax
import jax.numpy as jnp
from jax import lax
from jax.experimental import pallas as pl
from jax.experimental.pallas import tpu as pltpu
from jax.sharding import Mesh
from jax.sharding import PartitionSpec as P

BLK = ("blk_0", "blk_1", "blk_2", "blk_3")
AXES = ("blk_0", "blk_1", "blk_2", "blk_3", "mp")
MESH = pl.DeviceIdType.MESH
f32 = jnp.float32
bf16 = jnp.bfloat16
mix_third = 1.0 / 3.0
step_size = 0.1

CHUNKS = (64, 32, 32)
TILE = 1024


def folded(value):
    rows, cols = value.shape
    total = None
    for i in range(0, rows, 8):
        for j in range(0, cols, 128):
            part = value[i : i + 8, j : j + 128]
            total = part if total is None else total + part
    return total


def kernel(dims, p_ref, h_ref, t_ref, out_ref, err_ref, *scratch):
    ny, nz, rows, width, tok, chunks = dims
    n = len(chunks)
    names = iter(scratch)
    H, TG, TT, EA, ES, ER, EZ, EY = (next(names) for _ in range(8))
    X0, X1, XH, G0, X2, ZS, ZR, RA, RB = ([next(names) for _ in range(n)] for _ in range(9))
    h_s, h_r, t_s, t_r, x_s, x_r, z_s, z_r, o_s, o_r, e_s, e_r, loc = names

    y, z = lax.axis_index("blk_0"), lax.axis_index("blk_1")
    xh, c, xl = lax.axis_index("blk_2"), lax.axis_index("blk_3"), lax.axis_index("mp")
    x = 2 * xh + xl
    b = 2 * x + c
    mine = 2 * xh + c
    k = y * nz + z
    starts = [sum(chunks[:j]) for j in range(n)]

    def ring(dx, dc):
        xd = lax.rem(x + dx, 4)
        return {"blk_2": lax.div(xd, 2), "mp": lax.rem(xd, 2), "blk_3": lax.rem(c + dc, 2)}

    def group(dk):
        kd = lax.rem(k + dk + ny * nz, ny * nz)
        return {"blk_0": lax.div(kd, nz), "blk_1": lax.rem(kd, nz)}

    def remote(src, dst, send, recv, to):
        return pltpu.make_async_remote_copy(
            src_ref=src, dst_ref=dst, send_sem=send, recv_sem=recv, device_id=to, device_id_type=MESH
        )

    offsets = [(2, 0), (2, 1), (1, 0), (3, 0), (1, 1), (3, 1), (0, 1)]
    partners = [ring(*o) for o in offsets] + [group(1), group(-1)]
    partners += [{"blk_1": lax.rem(z + d, nz)} for d in range(1, nz)]
    partners += [{"blk_0": lax.rem(y + d, ny)} for d in range(1, ny)]
    barrier = pltpu.get_barrier_semaphore()
    for to in partners:
        pl.semaphore_signal(barrier, inc=1, device_id=to, device_id_type=MESH)

    def slot(dx):
        xs = lax.rem(x + dx, 4)
        return (2 * lax.div(xs, 2) + c) * 2 + lax.rem(xs, 2)

    half = tok // 2
    first, second, whole = pl.ds(0, half), pl.ds(half, half), pl.ds(0, tok)

    def hidden_copy(i, dx, part, to, own=False):
        dst = H.at[slot(dx), part]
        return remote(h_ref.at[part] if own else dst, dst, h_s.at[i], h_r.at[i], to)

    ahead, behind, sibling = ring(1, 0), ring(3, 0), ring(0, 1)
    own_h = [
        hidden_copy(0, 0, first, ahead, True),
        hidden_copy(1, 0, second, behind, True),
        hidden_copy(2, 0, second, ahead, True),
        hidden_copy(3, 0, first, behind, True),
        hidden_copy(4, 0, whole, sibling, True),
    ]
    relay_h = [hidden_copy(5, 3, first, ahead), hidden_copy(6, 1, second, behind)]
    pass_h = [
        hidden_copy(7, 3, whole, sibling),
        hidden_copy(8, 1, whole, sibling),
        hidden_copy(9, 2, first, sibling),
        hidden_copy(10, 2, second, sibling),
    ]
    keep_h = pltpu.make_async_copy(h_ref, H.at[slot(0)], loc.at[0])

    lane = rows
    t_copies = []
    for m in range(4):
        xd, cd = 2 * xl + m // 2, m % 2
        src = t_ref.at[:, pl.ds(m * lane, lane)]
        own = jnp.logical_and(x == xd, c == cd)
        to = {"blk_2": lax.div(xd, 2), "mp": lax.rem(xd, 2), "blk_3": cd}
        t_copies.append(
            (
                own,
                remote(src, TG.at[mine], t_s.at[m], t_r.at[mine], to),
                pltpu.make_async_copy(src, TG.at[mine], loc.at[1]),
            )
        )

    def x_copies(j):
        out = []
        for i, (dx, dc) in enumerate(offsets):
            bd = 2 * lax.rem(x + dx, 4) + lax.rem(c + dc, 2)
            src = p_ref.at[pl.ds(pl.multiple_of(bd * rows + starts[j], 16), chunks[j])]
            out.append(remote(src, X0[j].at[1 + mine, xl], x_s.at[j, i], x_r.at[j, i], ring(dx, dc)))
        src = p_ref.at[pl.ds(pl.multiple_of(b * rows + starts[j], 16), chunks[j])]
        return out, pltpu.make_async_copy(src, X0[j].at[1 + mine, xl], loc.at[2 + j])

    x0 = [x_copies(j) for j in range(n)]

    def halo(j, q, direction, src, dst):
        return remote(src, dst, z_s.at[j, q, direction], z_r.at[j, q, direction], group(1 - 2 * direction))

    x0_halo = [
        (halo(j, 0, 0, X0[j].at[4], X0[j].at[0]), halo(j, 0, 1, X0[j].at[1], X0[j].at[5])) for j in range(n)
    ]
    z_halo = [
        (halo(j, 1, 0, ZS[j].at[0], ZR[j].at[1]), halo(j, 1, 1, ZS[j].at[1], ZR[j].at[0])) for j in range(n)
    ]
    x1_halo = [
        (halo(j, 2, 0, X1[j].at[3, 1], XH[j].at[1]), halo(j, 2, 1, X1[j].at[0, 0], XH[j].at[0])) for j in range(n)
    ]

    def back_copies(j):
        out = []
        for s in range(8):
            r, hf = s // 2, s % 2
            own = jnp.logical_and(x == 2 * (r // 2) + hf, c == r % 2)
            to = {"blk_2": r // 2, "mp": hf, "blk_3": r % 2}
            dst = out_ref.at[pl.ds(pl.multiple_of(b * rows + starts[j], 16), chunks[j])]
            out.append(
                (
                    own,
                    remote(X2[j].at[r, hf], dst, o_s.at[j, s], o_r.at[j, b], to),
                    pltpu.make_async_copy(X2[j].at[r, hf], dst, loc.at[2 + n + j]),
                )
            )
        return out

    back = [back_copies(j) for j in range(n)]

    def start_one(entry):
        own, away, near = entry
        pl.when(jnp.logical_not(own))(away.start)
        pl.when(own)(near.start)

    def finish_one(entry):
        own, away, near = entry
        pl.when(jnp.logical_not(own))(away.wait_send)
        pl.when(own)(near.wait)

    def forward(w_ref, base, t_start, size, out):
        def replica(r, carry):
            def part(hf, acc):
                return acc + lax.dot_general(
                    w_ref[r + base, hf], H[2 * r + hf], (((1,), (1,)), ((), ())), preferred_element_type=f32
                )

            acc = lax.fori_loop(0, 2, part, jnp.zeros((size, tok), f32))
            out[r] = (acc - TT[r, pl.ds(t_start, size)]).astype(bf16)
            return carry

        lax.fori_loop(0, 4, replica, 0)

    tiles = width // TILE

    def over_tiles(body):
        def step(i, carry):
            ii = lax.div(i, 2 * tiles)
            hf = lax.rem(lax.div(i, tiles), 2)
            cols = pl.ds(pl.multiple_of(lax.rem(i, tiles) * TILE, TILE), TILE)
            body(ii, hf, cols)
            return carry

        lax.fori_loop(0, 4 * tiles, step, 0)

    def grad(res, r, hf, cols):
        return lax.dot_general(
            res[r], H[2 * r + hf, :, cols], (((1,), (0,)), ((), ())), preferred_element_type=f32
        ) * (1.0 / tok)

    def update(j, r, hf, cols, where=None):
        g = grad(RA[j], r, hf, cols)
        G0[j][r, hf, :, cols] = g
        own = X0[j][r + 1, hf, :, cols].astype(f32)
        right = X0[j][r + 2, hf, :, cols].astype(f32)
        left = X0[j][r, hf, :, cols].astype(f32)
        diff = own - right
        EA[0] += folded(diff * diff)
        pull = step_size * g.astype(bf16).astype(f32)
        new = ((left + own + right) * mix_third - pull).astype(bf16)
        X1[j][r, hf, :, cols] = new
        if where is not None:
            ZS[j][where, hf, :, cols] = (new.astype(f32) - pull).astype(bf16)

    def stage_B(j):
        for copy in x0_halo[j]:
            copy.wait_recv()
        over_tiles(lambda i, hf, cols: update(j, 3 - 3 * i, hf, cols, i))
        for copy in z_halo[j] + x1_halo[j]:
            copy.start()
        over_tiles(lambda i, hf, cols: update(j, 1 + i, hf, cols))

    def inner(j, i, hf, cols):
        r = 1 + i
        own = X1[j][r, hf, :, cols].astype(f32)
        right = X1[j][r + 1, hf, :, cols].astype(f32)
        left = X1[j][r - 1, hf, :, cols].astype(f32)
        diff = own - right
        EA[1] += folded(diff * diff)
        g0 = G0[j][r, hf, :, cols]
        tracks = (
            G0[j][r - 1, hf, :, cols].astype(bf16).astype(f32)
            + g0.astype(bf16).astype(f32)
            + G0[j][r + 1, hf, :, cols].astype(bf16).astype(f32)
        )
        track = (tracks * mix_third + grad(RB[j], r, hf, cols) - g0).astype(bf16).astype(f32)
        X2[j][r, hf, :, cols] = ((left + own + right) * mix_third - step_size * track).astype(bf16)

    def outer(j, i, hf, cols):
        r, nb = 3 - 3 * i, 2 - i
        own = X1[j][r, hf, :, cols].astype(f32)
        near = X1[j][nb, hf, :, cols].astype(f32)
        far = XH[j][hf, :, cols].astype(f32)
        near_diff, far_diff = own - near, own - far
        near_weight = jnp.where(i == 1, 1.0, 0.0).astype(f32)
        far_weight = jnp.where(i == hf, 1.0, 0.0).astype(f32)
        EA[1] += folded(near_diff * near_diff) * near_weight + folded(far_diff * far_diff) * far_weight
        g0 = G0[j][r, hf, :, cols]
        tracks = g0.astype(bf16).astype(f32) + G0[j][nb, hf, :, cols].astype(bf16).astype(f32)
        mixed = (ZR[j][i, hf, :, cols].astype(f32) + own + near - step_size * tracks) * mix_third
        X2[j][r, hf, :, cols] = (mixed - step_size * (grad(RB[j], r, hf, cols) - g0)).astype(bf16)

    def stage_H(j):
        for copy in x0[j][0]:
            copy.wait_recv()
        x0[j][1].wait()
        for copy in x0_halo[j]:
            copy.start()

    def stage_A(j):
        forward(X0[j], 1, starts[j], chunks[j], RA[j])

    def stage_C(j):
        forward(X1[j], 0, starts[j], chunks[j], RB[j])

    def stage_I(j):
        over_tiles(functools.partial(inner, j))
        for s in (2, 3, 4, 5):
            start_one(back[j][s])

    def stage_O(j):
        for copy in z_halo[j] + x1_halo[j]:
            copy.wait_recv()
        over_tiles(functools.partial(outer, j))

    def send_outer(j):
        for s in (6, 7, 0, 1):
            start_one(back[j][s])

    def issue_x0(j):
        for copy in x0[j][0]:
            copy.start()
        x0[j][1].start()

    EA[...] = jnp.zeros_like(EA)
    pl.semaphore_wait(barrier, len(partners))

    issue_x0(0)
    for copy in own_h:
        copy.start()
    keep_h.start()
    for entry in t_copies:
        start_one(entry)
    stage_H(0)
    own_h[0].wait_recv()
    relay_h[0].start()
    own_h[1].wait_recv()
    relay_h[1].start()
    for j in range(1, n):
        issue_x0(j)
    for r in range(4):
        own = jnp.logical_and(r == mine, xl == xh)
        arrival = remote(TG.at[r], TG.at[r], t_s.at[0], t_r.at[r], sibling)
        pl.when(jnp.logical_not(own))(arrival.wait_recv)
    for entry in t_copies:
        finish_one(entry)

    def turn(r, carry):
        TT[r] = TG[r].astype(f32).T
        return carry

    lax.fori_loop(0, 4, turn, 0)
    own_h[2].wait_recv()
    pass_h[0].start()
    own_h[3].wait_recv()
    pass_h[1].start()
    relay_h[0].wait_recv()
    pass_h[2].start()
    relay_h[1].wait_recv()
    pass_h[3].start()
    own_h[4].wait_recv()
    for copy in pass_h:
        copy.wait_recv()
    keep_h.wait()

    stage_A(0)
    stage_B(0)
    stage_C(0)
    stage_I(0)
    for j in range(1, n):
        stage_H(j)
        stage_A(j)
        stage_B(j)
        stage_O(j - 1)
        send_outer(j - 1)
        stage_C(j)
        stage_I(j)
    stage_O(n - 1)

    sums = [jnp.sum(EA[i], axis=0, keepdims=True) for i in range(2)]
    row = lax.broadcasted_iota(jnp.int32, (8, 128), 0)
    ES[0] = jnp.where(row == 0, sums[0], jnp.where(row == 1, sums[1], 0.0))
    ER[b] = ES[0]
    e0 = []
    for i, (dx, dc) in enumerate(offsets):
        copy = remote(ES.at[0], ER.at[b], e_s.at[0, i], e_r.at[0, i], ring(dx, dc))
        copy.start()
        e0.append(copy)
    send_outer(n - 1)
    for copy in e0:
        copy.wait_recv()
    total = ER[0]
    for i in range(1, 8):
        total = total + ER[i]
    ES[1] = total
    EZ[z] = total
    e1 = []
    for d in range(1, nz):
        copy = remote(ES.at[1], EZ.at[z], e_s.at[1, d], e_r.at[1, d], {"blk_1": lax.rem(z + d, nz)})
        copy.start()
        e1.append(copy)
    for copy in e1:
        copy.wait_recv()
    total = EZ[0]
    for i in range(1, nz):
        total = total + EZ[i]
    ES[2] = total
    EY[y] = total
    e2 = []
    for d in range(1, ny):
        copy = remote(ES.at[2], EY.at[y], e_s.at[2, d], e_r.at[2, d], {"blk_0": lax.rem(y + d, ny)})
        copy.start()
        e2.append(copy)
    for copy in e2:
        copy.wait_recv()
    total = EY[0]
    for i in range(1, ny):
        total = total + EY[i]
    err_ref[...] = total

    for j in range(n):
        for s in range(8):
            arrival = remote(X2[j].at[0, 0], out_ref.at[pl.ds(starts[j], chunks[j])], o_s.at[j, 0], o_r.at[j, s], sibling)
            pl.when(s != b)(arrival.wait_recv)
    for copy in own_h + relay_h + pass_h + e0 + e1 + e2:
        copy.wait_send()
    for j in range(n):
        for copy in list(x0[j][0]) + list(x0_halo[j] + z_halo[j] + x1_halo[j]):
            copy.wait_send()
        for entry in back[j]:
            finish_one(entry)


def on_device(sizes, params, hidden, targets):
    ny, nz = sizes
    state, feats, targ = params[0], hidden[0], targets[0]
    depth, width = state.shape
    tok = feats.shape[0]
    rows = depth // 8
    n = len(CHUNKS)
    V, D = pltpu.VMEM, pltpu.SemaphoreType.DMA
    scratch = [
        V((8, tok, width), bf16),
        V((4, tok, rows), bf16),
        V((4, rows, tok), f32),
        V((2, 8, 128), f32),
        V((3, 8, 128), f32),
        V((8, 8, 128), f32),
        V((nz, 8, 128), f32),
        V((ny, 8, 128), f32),
    ]
    scratch += [V((6, 2, r, width), bf16) for r in CHUNKS]
    scratch += [V((4, 2, r, width), bf16) for r in CHUNKS]
    scratch += [V((2, r, width), bf16) for r in CHUNKS]
    scratch += [V((4, 2, r, width), f32) for r in CHUNKS]
    scratch += [V((4, 2, r, width), bf16) for r in CHUNKS]
    scratch += [V((2, 2, r, width), bf16) for r in CHUNKS]
    scratch += [V((2, 2, r, width), bf16) for r in CHUNKS]
    scratch += [V((4, r, tok), bf16) for r in CHUNKS]
    scratch += [V((4, r, tok), bf16) for r in CHUNKS]
    scratch += [D((11,)), D((11,)), D((4,)), D((4,)), D((n, 7)), D((n, 7)), D((n, 3, 2)), D((n, 3, 2))]
    scratch += [D((n, 8)), D((n, 8)), D((3, 8)), D((3, 8)), D((2 + 2 * n,))]
    anywhere = pl.BlockSpec(memory_space=pl.ANY)
    new_state, err = pl.pallas_call(
        functools.partial(kernel, (ny, nz, rows, width, tok, CHUNKS)),
        out_shape=(jax.ShapeDtypeStruct(state.shape, bf16), jax.ShapeDtypeStruct((8, 128), f32)),
        in_specs=[anywhere] * 3,
        out_specs=(anywhere, pl.BlockSpec(memory_space=pltpu.VMEM)),
        scratch_shapes=scratch,
        compiler_params=pltpu.CompilerParams(
            collective_id=0, has_side_effects=True, vmem_limit_bytes=60 * 2**20
        ),
    )(state, feats, targ)
    errors = jnp.sum(err[:2], axis=1) / (2 * width * 4 * ny * nz)
    return (new_state[None], errors)


def solution(mesh):
    torus = Mesh(mesh.devices.reshape(4, 8, 2, 2, mesh.shape["mp"]), AXES)
    placed = (P(BLK, None, "mp"), P(BLK, None, "mp"), P(BLK, None, "mp"))
    return jax.shard_map(
        functools.partial(on_device, (4, 8)),
        mesh=torus,
        in_specs=placed,
        out_specs=(P(BLK, None, "mp"), P()),
        check_vma=False,
    )
```

```python
import functools

import jax
import jax.numpy as jnp
from jax import lax
from jax.experimental import pallas as pl
from jax.experimental.pallas import tpu as pltpu
from jax.sharding import Mesh
from jax.sharding import PartitionSpec as P

BLK = ("blk_0", "blk_1", "blk_2", "blk_3")
AXES = ("blk_0", "blk_1", "blk_2", "blk_3", "mp")
MESH = pl.DeviceIdType.MESH
f32 = jnp.float32
bf16 = jnp.bfloat16
mix_third = 1.0 / 3.0
step_size = 0.1

CHUNKS = (32, 48, 48)
TILE = 2048
ORDER = ("C0", "I0", "H1", "O0", "A1", "B1", "H2", "C1", "I1", "O1", "A2", "B2", "C2", "I2")


def folded(value):
    rows, cols = value.shape
    total = None
    for i in range(0, rows, 8):
        for j in range(0, cols, 128):
            part = value[i : i + 8, j : j + 128]
            total = part if total is None else total + part
    return total


def kernel(dims, p_ref, h_ref, t_ref, out_ref, err_ref, *scratch):
    ny, nz, rows, width, tok, chunks = dims
    n = len(chunks)
    names = iter(scratch)
    H, TG, TT, EA, ES, ER, EZ, EY = (next(names) for _ in range(8))
    X0, X1, XH, G0, X2, ZS, ZR, RA, RB = ([next(names) for _ in range(n)] for _ in range(9))
    h_s, h_r, t_s, t_r, x_s, x_r, z_s, z_r, o_s, o_r, e_s, e_r, loc = names

    y, z = lax.axis_index("blk_0"), lax.axis_index("blk_1")
    xh, c, xl = lax.axis_index("blk_2"), lax.axis_index("blk_3"), lax.axis_index("mp")
    x = 2 * xh + xl
    b = 2 * x + c
    mine = 2 * xh + c
    k = y * nz + z
    starts = [sum(chunks[:j]) for j in range(n)]

    def ring(dx, dc):
        xd = lax.rem(x + dx, 4)
        return {"blk_2": lax.div(xd, 2), "mp": lax.rem(xd, 2), "blk_3": lax.rem(c + dc, 2)}

    def group(dk):
        kd = lax.rem(k + dk + ny * nz, ny * nz)
        return {"blk_0": lax.div(kd, nz), "blk_1": lax.rem(kd, nz)}

    def remote(src, dst, send, recv, to):
        return pltpu.make_async_remote_copy(
            src_ref=src, dst_ref=dst, send_sem=send, recv_sem=recv, device_id=to, device_id_type=MESH
        )

    offsets = [(2, 0), (2, 1), (1, 0), (3, 0), (1, 1), (3, 1), (0, 1)]
    partners = [ring(*o) for o in offsets] + [group(1), group(-1)]
    partners += [{"blk_1": lax.rem(z + d, nz)} for d in range(1, nz)]
    partners += [{"blk_0": lax.rem(y + d, ny)} for d in range(1, ny)]
    barrier = pltpu.get_barrier_semaphore()
    for to in partners:
        pl.semaphore_signal(barrier, inc=1, device_id=to, device_id_type=MESH)

    def slot(dx):
        xs = lax.rem(x + dx, 4)
        return (2 * lax.div(xs, 2) + c) * 2 + lax.rem(xs, 2)

    half = tok // 2
    first, second, whole = pl.ds(0, half), pl.ds(half, half), pl.ds(0, tok)

    def hidden_copy(i, dx, part, to, own=False):
        dst = H.at[slot(dx), part]
        return remote(h_ref.at[part] if own else dst, dst, h_s.at[i], h_r.at[i], to)

    ahead, behind, sibling = ring(1, 0), ring(3, 0), ring(0, 1)
    own_h = [
        hidden_copy(0, 0, first, ahead, True),
        hidden_copy(1, 0, second, behind, True),
        hidden_copy(2, 0, second, ahead, True),
        hidden_copy(3, 0, first, behind, True),
        hidden_copy(4, 0, whole, sibling, True),
    ]
    relay_h = [hidden_copy(5, 3, first, ahead), hidden_copy(6, 1, second, behind)]
    pass_h = [
        hidden_copy(7, 3, whole, sibling),
        hidden_copy(8, 1, whole, sibling),
        hidden_copy(9, 2, first, sibling),
        hidden_copy(10, 2, second, sibling),
    ]
    keep_h = pltpu.make_async_copy(h_ref, H.at[slot(0)], loc.at[0])

    lane = rows
    t_copies = []
    for m in range(4):
        xd, cd = 2 * xl + m // 2, m % 2
        src = t_ref.at[:, pl.ds(m * lane, lane)]
        own = jnp.logical_and(x == xd, c == cd)
        to = {"blk_2": lax.div(xd, 2), "mp": lax.rem(xd, 2), "blk_3": cd}
        t_copies.append(
            (
                own,
                remote(src, TG.at[mine], t_s.at[m], t_r.at[mine], to),
                pltpu.make_async_copy(src, TG.at[mine], loc.at[1]),
            )
        )

    def x_copies(j):
        out = []
        for i, (dx, dc) in enumerate(offsets):
            bd = 2 * lax.rem(x + dx, 4) + lax.rem(c + dc, 2)
            src = p_ref.at[pl.ds(pl.multiple_of(bd * rows + starts[j], 16), chunks[j])]
            out.append(remote(src, X0[j].at[1 + mine, xl], x_s.at[j, i], x_r.at[j, i], ring(dx, dc)))
        src = p_ref.at[pl.ds(pl.multiple_of(b * rows + starts[j], 16), chunks[j])]
        return out, pltpu.make_async_copy(src, X0[j].at[1 + mine, xl], loc.at[2 + j])

    x0 = [x_copies(j) for j in range(n)]

    def halo(j, q, direction, src, dst):
        return remote(src, dst, z_s.at[j, q, direction], z_r.at[j, q, direction], group(1 - 2 * direction))

    x0_halo = [
        (halo(j, 0, 0, X0[j].at[4], X0[j].at[0]), halo(j, 0, 1, X0[j].at[1], X0[j].at[5])) for j in range(n)
    ]
    z_halo = [
        (halo(j, 1, 0, ZS[j].at[0], ZR[j].at[1]), halo(j, 1, 1, ZS[j].at[1], ZR[j].at[0])) for j in range(n)
    ]
    x1_halo = [
        (halo(j, 2, 0, X1[j].at[3, 1], XH[j].at[1]), halo(j, 2, 1, X1[j].at[0, 0], XH[j].at[0])) for j in range(n)
    ]

    def back_copies(j):
        out = []
        for s in range(8):
            r, hf = s // 2, s % 2
            own = jnp.logical_and(x == 2 * (r // 2) + hf, c == r % 2)
            to = {"blk_2": r // 2, "mp": hf, "blk_3": r % 2}
            dst = out_ref.at[pl.ds(pl.multiple_of(b * rows + starts[j], 16), chunks[j])]
            out.append(
                (
                    own,
                    remote(X2[j].at[r, hf], dst, o_s.at[j, s], o_r.at[j, b], to),
                    pltpu.make_async_copy(X2[j].at[r, hf], dst, loc.at[2 + n + j]),
                )
            )
        return out

    back = [back_copies(j) for j in range(n)]

    def start_one(entry):
        own, away, near = entry
        pl.when(jnp.logical_not(own))(away.start)
        pl.when(own)(near.start)

    def finish_one(entry):
        own, away, near = entry
        pl.when(jnp.logical_not(own))(away.wait_send)
        pl.when(own)(near.wait)

    def forward(w_ref, base, t_start, size, out, first=0, count=4):
        def replica(i, carry):
            r = first + i

            def part(hf, acc):
                return acc + lax.dot_general(
                    w_ref[r + base, hf], H[2 * r + hf], (((1,), (1,)), ((), ())), preferred_element_type=f32
                )

            acc = lax.fori_loop(0, 2, part, jnp.zeros((size, tok), f32))
            out[r] = (acc - TT[r, pl.ds(t_start, size)]).astype(bf16)
            return carry

        lax.fori_loop(0, count, replica, 0)

    tiles = width // TILE

    def over_tiles(body, count=2):
        def step(i, carry):
            ii = lax.div(i, 2 * tiles)
            hf = lax.rem(lax.div(i, tiles), 2)
            cols = pl.ds(pl.multiple_of(lax.rem(i, tiles) * TILE, TILE), TILE)
            body(ii, hf, cols)
            return carry

        lax.fori_loop(0, 2 * count * tiles, step, 0)

    def grad(res, r, hf, cols):
        return lax.dot_general(
            res[r], H[2 * r + hf, :, cols], (((1,), (0,)), ((), ())), preferred_element_type=f32
        ) * (1.0 / tok)

    def update(j, r, hf, cols, where=None):
        g = grad(RA[j], r, hf, cols)
        G0[j][r, hf, :, cols] = g
        own = X0[j][r + 1, hf, :, cols].astype(f32)
        right = X0[j][r + 2, hf, :, cols].astype(f32)
        left = X0[j][r, hf, :, cols].astype(f32)
        diff = own - right
        EA[0] += folded(diff * diff)
        pull = step_size * g.astype(bf16).astype(f32)
        new = ((left + own + right) * mix_third - pull).astype(bf16)
        X1[j][r, hf, :, cols] = new
        if where is not None:
            ZS[j][where, hf, :, cols] = (new.astype(f32) - pull).astype(bf16)

    def stage_B(j):
        for copy in x0_halo[j]:
            copy.wait_recv()
        over_tiles(lambda i, hf, cols: update(j, 3 - 3 * i, hf, cols, i))
        for copy in z_halo[j] + x1_halo[j]:
            copy.start()
        over_tiles(lambda i, hf, cols: update(j, 1 + i, hf, cols))

    def pair(side):
        forward(X0[0], 1, 0, chunks[0], RA[0], 2 * side, 2)
        edge = 1 - side
        over_tiles(lambda i, hf, cols: update(0, 3 * side, hf, cols, edge), 1)
        for way in range(2):

            @pl.when(edge == way)
            def _():
                z_halo[0][way].start()
                x1_halo[0][way].start()

        over_tiles(lambda i, hf, cols: update(0, 1 + side, hf, cols), 1)

    def inner(j, i, hf, cols):
        r = 1 + i
        own = X1[j][r, hf, :, cols].astype(f32)
        right = X1[j][r + 1, hf, :, cols].astype(f32)
        left = X1[j][r - 1, hf, :, cols].astype(f32)
        diff = own - right
        EA[1] += folded(diff * diff)
        g0 = G0[j][r, hf, :, cols]
        tracks = (
            G0[j][r - 1, hf, :, cols].astype(bf16).astype(f32)
            + g0.astype(bf16).astype(f32)
            + G0[j][r + 1, hf, :, cols].astype(bf16).astype(f32)
        )
        track = (tracks * mix_third + grad(RB[j], r, hf, cols) - g0).astype(bf16).astype(f32)
        X2[j][r, hf, :, cols] = ((left + own + right) * mix_third - step_size * track).astype(bf16)

    def outer(j, i, hf, cols):
        r, nb = 3 - 3 * i, 2 - i
        own = X1[j][r, hf, :, cols].astype(f32)
        near = X1[j][nb, hf, :, cols].astype(f32)
        far = XH[j][hf, :, cols].astype(f32)
        near_diff, far_diff = own - near, own - far
        near_weight = jnp.where(i == 1, 1.0, 0.0).astype(f32)
        far_weight = jnp.where(i == hf, 1.0, 0.0).astype(f32)
        EA[1] += folded(near_diff * near_diff) * near_weight + folded(far_diff * far_diff) * far_weight
        g0 = G0[j][r, hf, :, cols]
        tracks = g0.astype(bf16).astype(f32) + G0[j][nb, hf, :, cols].astype(bf16).astype(f32)
        mixed = (ZR[j][i, hf, :, cols].astype(f32) + own + near - step_size * tracks) * mix_third
        X2[j][r, hf, :, cols] = (mixed - step_size * (grad(RB[j], r, hf, cols) - g0)).astype(bf16)

    def stage_H(j):
        for copy in x0[j][0]:
            copy.wait_recv()
        x0[j][1].wait()
        for copy in x0_halo[j]:
            copy.start()

    def stage_A(j):
        forward(X0[j], 1, starts[j], chunks[j], RA[j])

    def stage_C(j):
        forward(X1[j], 0, starts[j], chunks[j], RB[j])

    def stage_I(j):
        over_tiles(functools.partial(inner, j))
        for s in (2, 3, 4, 5):
            start_one(back[j][s])

    def stage_O(j):
        for copy in z_halo[j] + x1_halo[j]:
            copy.wait_recv()
        over_tiles(functools.partial(outer, j))

    def send_outer(j):
        for s in (6, 7, 0, 1):
            start_one(back[j][s])

    def issue_x0(j):
        for copy in x0[j][0]:
            copy.start()
        x0[j][1].start()

    EA[...] = jnp.zeros_like(EA)
    pl.semaphore_wait(barrier, len(partners))

    issue_x0(0)
    for copy in own_h:
        copy.start()
    keep_h.start()
    for entry in t_copies:
        start_one(entry)
    stage_H(0)
    own_h[0].wait_recv()
    relay_h[0].start()
    own_h[1].wait_recv()
    relay_h[1].start()
    for j in range(1, n):
        issue_x0(j)
    for r in range(4):
        own = jnp.logical_and(r == mine, xl == xh)
        arrival = remote(TG.at[r], TG.at[r], t_s.at[0], t_r.at[r], sibling)
        pl.when(jnp.logical_not(own))(arrival.wait_recv)
    for entry in t_copies:
        finish_one(entry)

    def turn(r, carry):
        TT[r] = TG[r].astype(f32).T
        return carry

    lax.fori_loop(0, 4, turn, 0)
    own_h[2].wait_recv()
    pass_h[0].start()
    own_h[3].wait_recv()
    pass_h[1].start()
    own_h[4].wait_recv()
    keep_h.wait()
    pass_h[0].wait_recv()
    pass_h[1].wait_recv()
    for copy in x0_halo[0]:
        copy.wait_recv()
    pair(xh)
    relay_h[0].wait_recv()
    pass_h[2].start()
    relay_h[1].wait_recv()
    pass_h[3].start()
    pass_h[2].wait_recv()
    pass_h[3].wait_recv()
    pair(1 - xh)

    stages = {"H": stage_H, "A": stage_A, "B": stage_B, "C": stage_C, "I": stage_I, "O": stage_O}
    for step in ORDER:
        stages[step[0]](int(step[1]))
        if step[0] == "O":
            send_outer(int(step[1]))
    stage_O(n - 1)

    sums = [jnp.sum(EA[i], axis=0, keepdims=True) for i in range(2)]
    row = lax.broadcasted_iota(jnp.int32, (8, 128), 0)
    ES[0] = jnp.where(row == 0, sums[0], jnp.where(row == 1, sums[1], 0.0))
    ER[b] = ES[0]
    e0 = []
    for i, (dx, dc) in enumerate(offsets):
        copy = remote(ES.at[0], ER.at[b], e_s.at[0, i], e_r.at[0, i], ring(dx, dc))
        copy.start()
        e0.append(copy)
    send_outer(n - 1)
    for copy in e0:
        copy.wait_recv()
    total = ER[0]
    for i in range(1, 8):
        total = total + ER[i]
    ES[1] = total
    EZ[z] = total
    e1 = []
    for d in range(1, nz):
        copy = remote(ES.at[1], EZ.at[z], e_s.at[1, d], e_r.at[1, d], {"blk_1": lax.rem(z + d, nz)})
        copy.start()
        e1.append(copy)
    for copy in e1:
        copy.wait_recv()
    total = EZ[0]
    for i in range(1, nz):
        total = total + EZ[i]
    ES[2] = total
    EY[y] = total
    e2 = []
    for d in range(1, ny):
        copy = remote(ES.at[2], EY.at[y], e_s.at[2, d], e_r.at[2, d], {"blk_0": lax.rem(y + d, ny)})
        copy.start()
        e2.append(copy)
    for copy in e2:
        copy.wait_recv()
    total = EY[0]
    for i in range(1, ny):
        total = total + EY[i]
    for i in range(2):
        err_ref[i] = jnp.sum(total[i : i + 1]) / (2 * width * 4 * ny * nz)

    for j in range(n):
        for s in range(8):
            arrival = remote(X2[j].at[0, 0], out_ref.at[pl.ds(starts[j], chunks[j])], o_s.at[j, 0], o_r.at[j, s], sibling)
            pl.when(s != b)(arrival.wait_recv)
    for copy in own_h + relay_h + pass_h + e0 + e1 + e2:
        copy.wait_send()
    for j in range(n):
        for copy in list(x0[j][0]) + list(x0_halo[j] + z_halo[j] + x1_halo[j]):
            copy.wait_send()
        for entry in back[j]:
            finish_one(entry)


def settle(src, dst, hold, s_in, s_out):
    parts = 8
    size = src.shape[0] // parts
    loads = [
        pltpu.make_async_copy(src.at[pl.ds(i * size, size)], hold.at[pl.ds(i * size, size)], s_in.at[i])
        for i in range(parts)
    ]
    stores = [
        pltpu.make_async_copy(hold.at[pl.ds(i * size, size)], dst.at[pl.ds(i * size, size)], s_out.at[i])
        for i in range(parts)
    ]
    for load in loads:
        load.start()
    for load, store in zip(loads, stores):
        load.wait()
        store.start()
    for store in stores:
        store.wait()


def on_device(sizes, params, hidden, targets):
    ny, nz = sizes
    state, feats, targ = params[0], hidden[0], targets[0]
    depth, width = state.shape
    tok = feats.shape[0]
    rows = depth // 8
    n = len(CHUNKS)
    V, D = pltpu.VMEM, pltpu.SemaphoreType.DMA
    scratch = [
        V((8, tok, width), bf16),
        V((4, tok, rows), bf16),
        V((4, rows, tok), f32),
        V((2, 8, 128), f32),
        V((3, 8, 128), f32),
        V((8, 8, 128), f32),
        V((nz, 8, 128), f32),
        V((ny, 8, 128), f32),
    ]
    scratch += [V((6, 2, r, width), bf16) for r in CHUNKS]
    scratch += [V((4, 2, r, width), bf16) for r in CHUNKS]
    scratch += [V((2, r, width), bf16) for r in CHUNKS]
    scratch += [V((4, 2, r, width), f32) for r in CHUNKS]
    scratch += [V((4, 2, r, width), bf16) for r in CHUNKS]
    scratch += [V((2, 2, r, width), bf16) for r in CHUNKS]
    scratch += [V((2, 2, r, width), bf16) for r in CHUNKS]
    scratch += [V((4, r, tok), bf16) for r in CHUNKS]
    scratch += [V((4, r, tok), bf16) for r in CHUNKS]
    scratch += [D((11,)), D((11,)), D((4,)), D((4,)), D((n, 7)), D((n, 7)), D((n, 3, 2)), D((n, 3, 2))]
    scratch += [D((n, 8)), D((n, 8)), D((3, 8)), D((3, 8)), D((2 + 2 * n,))]
    anywhere = pl.BlockSpec(memory_space=pl.ANY)
    new_state, errors = pl.pallas_call(
        functools.partial(kernel, (ny, nz, rows, width, tok, CHUNKS)),
        out_shape=(jax.ShapeDtypeStruct(state.shape, bf16), jax.ShapeDtypeStruct((2,), f32)),
        in_specs=[anywhere] * 3,
        out_specs=(anywhere, pl.BlockSpec(memory_space=pltpu.SMEM)),
        scratch_shapes=scratch,
        compiler_params=pltpu.CompilerParams(
            collective_id=0, has_side_effects=True, vmem_limit_bytes=60 * 2**20
        ),
    )(state, feats, targ)
    new_state = pl.pallas_call(
        settle,
        out_shape=jax.ShapeDtypeStruct(state.shape, bf16),
        in_specs=[anywhere],
        out_specs=anywhere,
        scratch_shapes=[V(state.shape, bf16), D((8,)), D((8,))],
    )(new_state)
    return (new_state[None], errors)


def solution(mesh):
    torus = Mesh(mesh.devices.reshape(4, 8, 2, 2, mesh.shape["mp"]), AXES)
    placed = (P(BLK, None, "mp"), P(BLK, None, "mp"), P(BLK, None, "mp"))
    return jax.shard_map(
        functools.partial(on_device, (4, 8)),
        mesh=torus,
        in_specs=placed,
        out_specs=(P(BLK, None, "mp"), P()),
        check_vma=False,
    )
```

```python
import functools

import jax
import jax.numpy as jnp
from jax import lax
from jax.experimental import pallas as pl
from jax.experimental.pallas import tpu as pltpu
from jax.sharding import Mesh
from jax.sharding import PartitionSpec as P

BLK = ("blk_0", "blk_1", "blk_2", "blk_3")
AXES = ("blk_0", "blk_1", "blk_2", "blk_3", "mp")
MESH = pl.DeviceIdType.MESH
f32 = jnp.float32
bf16 = jnp.bfloat16
mix_third = 1.0 / 3.0
step_size = 0.1

CHUNKS = (32, 48, 48)
TILE = 2048
ORDER = ("F0", "J0", "H2", "P0", "F1", "J1", "U2", "C2", "I2", "O1")
EARLY = 2


def folded(value):
    rows, cols = value.shape
    total = None
    for i in range(0, rows, 8):
        for j in range(0, cols, 128):
            part = value[i : i + 8, j : j + 128]
            total = part if total is None else total + part
    return total


def kernel(dims, p_ref, h_ref, t_ref, out_ref, err_ref, *scratch):
    ny, nz, rows, width, tok, chunks = dims
    n = len(chunks)
    names = iter(scratch)
    H, TG, TT, EA, ES, ER, EZ, EY = (next(names) for _ in range(8))
    X0, X1, XH, G0, X2, ZS, ZR, RA, RB = ([next(names) for _ in range(n)] for _ in range(9))
    h_s, h_r, t_s, t_r, x_s, x_r, z_s, z_r, o_s, o_r, e_s, e_r, loc = names

    y, z = lax.axis_index("blk_0"), lax.axis_index("blk_1")
    xh, c, xl = lax.axis_index("blk_2"), lax.axis_index("blk_3"), lax.axis_index("mp")
    x = 2 * xh + xl
    b = 2 * x + c
    mine = 2 * xh + c
    k = y * nz + z
    starts = [sum(chunks[:j]) for j in range(n)]

    def ring(dx, dc):
        xd = lax.rem(x + dx, 4)
        return {"blk_2": lax.div(xd, 2), "mp": lax.rem(xd, 2), "blk_3": lax.rem(c + dc, 2)}

    def group(dk):
        kd = lax.rem(k + dk + ny * nz, ny * nz)
        return {"blk_0": lax.div(kd, nz), "blk_1": lax.rem(kd, nz)}

    def remote(src, dst, send, recv, to):
        return pltpu.make_async_remote_copy(
            src_ref=src, dst_ref=dst, send_sem=send, recv_sem=recv, device_id=to, device_id_type=MESH
        )

    offsets = [(2, 0), (2, 1), (1, 0), (3, 0), (1, 1), (3, 1), (0, 1)]
    partners = [ring(*o) for o in offsets] + [group(1), group(-1)]
    partners += [{"blk_1": lax.rem(z + d, nz)} for d in range(1, nz)]
    partners += [{"blk_0": lax.rem(y + d, ny)} for d in range(1, ny)]
    barrier = pltpu.get_barrier_semaphore()
    for to in partners:
        pl.semaphore_signal(barrier, inc=1, device_id=to, device_id_type=MESH)

    def slot(dx):
        xs = lax.rem(x + dx, 4)
        return (2 * lax.div(xs, 2) + c) * 2 + lax.rem(xs, 2)

    half = tok // 2
    first, second, whole = pl.ds(0, half), pl.ds(half, half), pl.ds(0, tok)

    def hidden_copy(i, dx, part, to, own=False):
        dst = H.at[slot(dx), part]
        return remote(h_ref.at[part] if own else dst, dst, h_s.at[i], h_r.at[i], to)

    ahead, behind, sibling = ring(1, 0), ring(3, 0), ring(0, 1)
    own_h = [
        hidden_copy(0, 0, first, ahead, True),
        hidden_copy(1, 0, second, behind, True),
        hidden_copy(2, 0, second, ahead, True),
        hidden_copy(3, 0, first, behind, True),
        hidden_copy(4, 0, whole, sibling, True),
    ]
    relay_h = [hidden_copy(5, 3, first, ahead), hidden_copy(6, 1, second, behind)]
    pass_h = [
        hidden_copy(7, 3, whole, sibling),
        hidden_copy(8, 1, whole, sibling),
        hidden_copy(9, 2, first, sibling),
        hidden_copy(10, 2, second, sibling),
    ]
    keep_h = pltpu.make_async_copy(h_ref, H.at[slot(0)], loc.at[0])

    lane = rows
    t_copies = []
    for m in range(4):
        xd, cd = 2 * xl + m // 2, m % 2
        src = t_ref.at[:, pl.ds(m * lane, lane)]
        own = jnp.logical_and(x == xd, c == cd)
        to = {"blk_2": lax.div(xd, 2), "mp": lax.rem(xd, 2), "blk_3": cd}
        t_copies.append(
            (
                own,
                remote(src, TG.at[mine], t_s.at[m], t_r.at[mine], to),
                pltpu.make_async_copy(src, TG.at[mine], loc.at[1]),
            )
        )

    def x_copies(j):
        out = []
        for i, (dx, dc) in enumerate(offsets):
            bd = 2 * lax.rem(x + dx, 4) + lax.rem(c + dc, 2)
            src = p_ref.at[pl.ds(pl.multiple_of(bd * rows + starts[j], 16), chunks[j])]
            out.append(remote(src, X0[j].at[1 + mine, xl], x_s.at[j, i], x_r.at[j, i], ring(dx, dc)))
        src = p_ref.at[pl.ds(pl.multiple_of(b * rows + starts[j], 16), chunks[j])]
        return out, pltpu.make_async_copy(src, X0[j].at[1 + mine, xl], loc.at[2 + j])

    x0 = [x_copies(j) for j in range(n)]

    def halo(j, q, direction, src, dst):
        return remote(src, dst, z_s.at[j, q, direction], z_r.at[j, q, direction], group(1 - 2 * direction))

    x0_halo = [
        (halo(j, 0, 0, X0[j].at[4], X0[j].at[0]), halo(j, 0, 1, X0[j].at[1], X0[j].at[5])) for j in range(n)
    ]
    z_halo = [
        (halo(j, 1, 0, ZS[j].at[0], ZR[j].at[1]), halo(j, 1, 1, ZS[j].at[1], ZR[j].at[0])) for j in range(n)
    ]
    x1_halo = [
        (halo(j, 2, 0, X1[j].at[3, 1], XH[j].at[1]), halo(j, 2, 1, X1[j].at[0, 0], XH[j].at[0])) for j in range(n)
    ]

    def back_copies(j):
        out = []
        for s in range(8):
            r, hf = s // 2, s % 2
            own = jnp.logical_and(x == 2 * (r // 2) + hf, c == r % 2)
            to = {"blk_2": r // 2, "mp": hf, "blk_3": r % 2}
            dst = out_ref.at[pl.ds(pl.multiple_of(b * rows + starts[j], 16), chunks[j])]
            out.append(
                (
                    own,
                    remote(X2[j].at[r, hf], dst, o_s.at[j, s], o_r.at[j, b], to),
                    pltpu.make_async_copy(X2[j].at[r, hf], dst, loc.at[2 + n + j]),
                )
            )
        return out

    back = [back_copies(j) for j in range(n)]

    def start_one(entry):
        own, away, near = entry
        pl.when(jnp.logical_not(own))(away.start)
        pl.when(own)(near.start)

    def finish_one(entry):
        own, away, near = entry
        pl.when(jnp.logical_not(own))(away.wait_send)
        pl.when(own)(near.wait)

    def forward(w_ref, base, t_start, size, out, first=0, count=4):
        def replica(i, carry):
            r = first + i

            def part(hf, acc):
                return acc + lax.dot_general(
                    w_ref[r + base, hf], H[2 * r + hf], (((1,), (1,)), ((), ())), preferred_element_type=f32
                )

            acc = lax.fori_loop(0, 2, part, jnp.zeros((size, tok), f32))
            out[r] = (acc - TT[r, pl.ds(t_start, size)]).astype(bf16)
            return carry

        lax.fori_loop(0, count, replica, 0)

    tiles = width // TILE

    def over_tiles(body, count=2):
        def step(i, carry):
            ii = lax.div(i, 2 * tiles)
            hf = lax.rem(lax.div(i, tiles), 2)
            cols = pl.ds(pl.multiple_of(lax.rem(i, tiles) * TILE, TILE), TILE)
            body(ii, hf, cols)
            return carry

        lax.fori_loop(0, 2 * count * tiles, step, 0)

    def grad(res, r, hf, cols):
        return lax.dot_general(
            res, H[2 * r + hf, :, cols], (((1,), (0,)), ((), ())), preferred_element_type=f32
        ) * (1.0 / tok)

    def update(j, r, hf, cols, where=None, g=None):
        g = grad(RA[j][r], r, hf, cols) if g is None else g
        G0[j][r, hf, :, cols] = g
        own = X0[j][r + 1, hf, :, cols].astype(f32)
        right = X0[j][r + 2, hf, :, cols].astype(f32)
        left = X0[j][r, hf, :, cols].astype(f32)
        diff = own - right
        EA[0] += folded(diff * diff)
        pull = step_size * g.astype(bf16).astype(f32)
        new = ((left + own + right) * mix_third - pull).astype(bf16)
        X1[j][r, hf, :, cols] = new
        if where is not None:
            ZS[j][where, hf, :, cols] = (new.astype(f32) - pull).astype(bf16)

    def stage_B(j):
        for copy in x0_halo[j]:
            copy.wait_recv()
        over_tiles(lambda i, hf, cols: update(j, 3 - 3 * i, hf, cols, i))
        for copy in z_halo[j] + x1_halo[j]:
            copy.start()
        over_tiles(lambda i, hf, cols: update(j, 1 + i, hf, cols))

    def pair(side):
        forward(X0[0], 1, 0, chunks[0], RA[0], 2 * side, 2)
        edge = 1 - side
        over_tiles(lambda i, hf, cols: update(0, 3 * side, hf, cols, edge), 1)
        for way in range(2):

            @pl.when(edge == way)
            def _():
                z_halo[0][way].start()
                x1_halo[0][way].start()

        over_tiles(lambda i, hf, cols: update(0, 1 + side, hf, cols), 1)

    def inner(j, i, hf, cols, g=None):
        r = 1 + i
        g = grad(RB[j][r], r, hf, cols) if g is None else g
        own = X1[j][r, hf, :, cols].astype(f32)
        right = X1[j][r + 1, hf, :, cols].astype(f32)
        left = X1[j][r - 1, hf, :, cols].astype(f32)
        diff = own - right
        EA[1] += folded(diff * diff)
        g0 = G0[j][r, hf, :, cols]
        tracks = (
            G0[j][r - 1, hf, :, cols].astype(bf16).astype(f32)
            + g0.astype(bf16).astype(f32)
            + G0[j][r + 1, hf, :, cols].astype(bf16).astype(f32)
        )
        track = (tracks * mix_third + g - g0).astype(bf16).astype(f32)
        X2[j][r, hf, :, cols] = ((left + own + right) * mix_third - step_size * track).astype(bf16)

    def outer(j, i, hf, cols, g=None):
        r, nb = 3 - 3 * i, 2 - i
        g = grad(RB[j][r], r, hf, cols) if g is None else g
        own = X1[j][r, hf, :, cols].astype(f32)
        near = X1[j][nb, hf, :, cols].astype(f32)
        far = XH[j][hf, :, cols].astype(f32)
        near_diff, far_diff = own - near, own - far
        near_weight = jnp.where(i == 1, 1.0, 0.0).astype(f32)
        far_weight = jnp.where(i == hf, 1.0, 0.0).astype(f32)
        EA[1] += folded(near_diff * near_diff) * near_weight + folded(far_diff * far_diff) * far_weight
        g0 = G0[j][r, hf, :, cols]
        tracks = g0.astype(bf16).astype(f32) + G0[j][nb, hf, :, cols].astype(bf16).astype(f32)
        mixed = (ZR[j][i, hf, :, cols].astype(f32) + own + near - step_size * tracks) * mix_third
        X2[j][r, hf, :, cols] = (mixed - step_size * (g - g0)).astype(bf16)

    def stage_H(j):
        for copy in x0[j][0]:
            copy.wait_recv()
        x0[j][1].wait()
        for copy in x0_halo[j]:
            copy.start()

    def stage_A(j):
        forward(X0[j], 1, starts[j], chunks[j], RA[j])

    def stage_C(j):
        forward(X1[j], 0, starts[j], chunks[j], RB[j])

    def stage_I(j):
        over_tiles(functools.partial(inner, j))
        for s in (2, 3, 4, 5):
            start_one(back[j][s])

    def stage_O(j):
        for copy in z_halo[j] + x1_halo[j]:
            copy.wait_recv()
        over_tiles(functools.partial(outer, j))

    def both(j, r, hf, cols):
        res = jnp.concatenate([RB[j][r], RA[j + 1][r]], axis=0)
        g = grad(res, r, hf, cols)
        return g[: chunks[j]], g[chunks[j] :]

    def stage_F(j):
        size = chunks[j]

        def replica(r, carry):
            def part(hf, acc):
                w = jnp.concatenate([X1[j][r, hf], X0[j + 1][r + 1, hf]], axis=0)
                return acc + lax.dot_general(w, H[2 * r + hf], (((1,), (1,)), ((), ())), preferred_element_type=f32)

            acc = lax.fori_loop(0, 2, part, jnp.zeros((size + chunks[j + 1], tok), f32))
            RB[j][r] = (acc[:size] - TT[r, pl.ds(starts[j], size)]).astype(bf16)
            RA[j + 1][r] = (acc[size:] - TT[r, pl.ds(starts[j + 1], chunks[j + 1])]).astype(bf16)
            return carry

        lax.fori_loop(0, 4, replica, 0)

    def stage_J(j):
        def body(i, hf, cols):
            g1, g0 = both(j, 1 + i, hf, cols)
            inner(j, i, hf, cols, g1)
            update(j + 1, 1 + i, hf, cols, None, g0)

        over_tiles(body)
        for s in (2, 3, 4, 5):
            start_one(back[j][s])

    def stage_P(j):
        for copy in z_halo[j] + x1_halo[j] + x0_halo[j + 1]:
            copy.wait_recv()

        def body(i, hf, cols):
            g1, g0 = both(j, 3 - 3 * i, hf, cols)
            outer(j, i, hf, cols, g1)
            update(j + 1, 3 - 3 * i, hf, cols, i, g0)

        over_tiles(body)
        for copy in z_halo[j + 1] + x1_halo[j + 1]:
            copy.start()
        send_outer(j)

    def stage_U(j):
        for copy in x0_halo[j]:
            copy.wait_recv()
        over_tiles(lambda i, hf, cols: update(j, 3 - 3 * i, hf, cols, i))
        for copy in z_halo[j] + x1_halo[j]:
            copy.start()

    def send_outer(j):
        for s in (6, 7, 0, 1):
            start_one(back[j][s])

    def issue_x0(j):
        for copy in x0[j][0]:
            copy.start()
        x0[j][1].start()

    EA[...] = jnp.zeros_like(EA)
    pl.semaphore_wait(barrier, len(partners))

    issue_x0(0)
    for copy in own_h:
        copy.start()
    keep_h.start()
    for entry in t_copies:
        start_one(entry)
    stage_H(0)
    own_h[0].wait_recv()
    for j in range(1, EARLY):
        issue_x0(j)
    relay_h[0].start()
    own_h[1].wait_recv()
    relay_h[1].start()
    for j in range(EARLY, n):
        issue_x0(j)
    for r in range(4):
        own = jnp.logical_and(r == mine, xl == xh)
        arrival = remote(TG.at[r], TG.at[r], t_s.at[0], t_r.at[r], sibling)
        pl.when(jnp.logical_not(own))(arrival.wait_recv)
    for entry in t_copies:
        finish_one(entry)

    def turn(r, carry):
        TT[r] = TG[r].astype(f32).T
        return carry

    lax.fori_loop(0, 4, turn, 0)
    own_h[2].wait_recv()
    pass_h[0].start()
    own_h[3].wait_recv()
    pass_h[1].start()
    own_h[4].wait_recv()
    keep_h.wait()
    pass_h[0].wait_recv()
    pass_h[1].wait_recv()
    for copy in x0_halo[0]:
        copy.wait_recv()
    pair(xh)
    for j in range(1, EARLY):
        stage_H(j)
    relay_h[0].wait_recv()
    pass_h[2].start()
    relay_h[1].wait_recv()
    pass_h[3].start()
    pass_h[2].wait_recv()
    pass_h[3].wait_recv()
    pair(1 - xh)

    stages = {"F": stage_F, "J": stage_J, "P": stage_P, "U": stage_U}
    stages |= {"H": stage_H, "A": stage_A, "B": stage_B, "C": stage_C, "I": stage_I, "O": stage_O}
    for step in ORDER:
        stages[step[0]](int(step[1]))
        if step[0] == "O":
            send_outer(int(step[1]))
    stage_O(n - 1)

    sums = [jnp.sum(EA[i], axis=0, keepdims=True) for i in range(2)]
    row = lax.broadcasted_iota(jnp.int32, (8, 128), 0)
    ES[0] = jnp.where(row == 0, sums[0], jnp.where(row == 1, sums[1], 0.0))
    ER[b] = ES[0]
    e0 = []
    for i, (dx, dc) in enumerate(offsets):
        copy = remote(ES.at[0], ER.at[b], e_s.at[0, i], e_r.at[0, i], ring(dx, dc))
        copy.start()
        e0.append(copy)
    send_outer(n - 1)
    for copy in e0:
        copy.wait_recv()
    total = ER[0]
    for i in range(1, 8):
        total = total + ER[i]
    ES[1] = total
    EZ[z] = total
    e1 = []
    for d in range(1, nz):
        copy = remote(ES.at[1], EZ.at[z], e_s.at[1, d], e_r.at[1, d], {"blk_1": lax.rem(z + d, nz)})
        copy.start()
        e1.append(copy)
    for copy in e1:
        copy.wait_recv()
    total = EZ[0]
    for i in range(1, nz):
        total = total + EZ[i]
    ES[2] = total
    EY[y] = total
    e2 = []
    for d in range(1, ny):
        copy = remote(ES.at[2], EY.at[y], e_s.at[2, d], e_r.at[2, d], {"blk_0": lax.rem(y + d, ny)})
        copy.start()
        e2.append(copy)
    for copy in e2:
        copy.wait_recv()
    total = EY[0]
    for i in range(1, ny):
        total = total + EY[i]
    for i in range(2):
        err_ref[i] = jnp.sum(total[i : i + 1]) / (2 * width * 4 * ny * nz)

    for j in range(n):
        for s in range(8):
            arrival = remote(X2[j].at[0, 0], out_ref.at[pl.ds(starts[j], chunks[j])], o_s.at[j, 0], o_r.at[j, s], sibling)
            pl.when(s != b)(arrival.wait_recv)
    for copy in own_h + relay_h + pass_h + e0 + e1 + e2:
        copy.wait_send()
    for j in range(n):
        for copy in list(x0[j][0]) + list(x0_halo[j] + z_halo[j] + x1_halo[j]):
            copy.wait_send()
        for entry in back[j]:
            finish_one(entry)


def settle(src, dst, hold, s_in, s_out):
    parts = 8
    size = src.shape[0] // parts
    loads = [
        pltpu.make_async_copy(src.at[pl.ds(i * size, size)], hold.at[pl.ds(i * size, size)], s_in.at[i])
        for i in range(parts)
    ]
    stores = [
        pltpu.make_async_copy(hold.at[pl.ds(i * size, size)], dst.at[pl.ds(i * size, size)], s_out.at[i])
        for i in range(parts)
    ]
    for load in loads:
        load.start()
    for load, store in zip(loads, stores):
        load.wait()
        store.start()
    for store in stores:
        store.wait()


def on_device(sizes, params, hidden, targets):
    ny, nz = sizes
    state, feats, targ = params[0], hidden[0], targets[0]
    depth, width = state.shape
    tok = feats.shape[0]
    rows = depth // 8
    n = len(CHUNKS)
    V, D = pltpu.VMEM, pltpu.SemaphoreType.DMA
    scratch = [
        V((8, tok, width), bf16),
        V((4, tok, rows), bf16),
        V((4, rows, tok), f32),
        V((2, 8, 128), f32),
        V((3, 8, 128), f32),
        V((8, 8, 128), f32),
        V((nz, 8, 128), f32),
        V((ny, 8, 128), f32),
    ]
    scratch += [V((6, 2, r, width), bf16) for r in CHUNKS]
    scratch += [V((4, 2, r, width), bf16) for r in CHUNKS]
    scratch += [V((2, r, width), bf16) for r in CHUNKS]
    scratch += [V((4, 2, r, width), f32) for r in CHUNKS]
    scratch += [V((4, 2, r, width), bf16) for r in CHUNKS]
    scratch += [V((2, 2, r, width), bf16) for r in CHUNKS]
    scratch += [V((2, 2, r, width), bf16) for r in CHUNKS]
    scratch += [V((4, r, tok), bf16) for r in CHUNKS]
    scratch += [V((4, r, tok), bf16) for r in CHUNKS]
    scratch += [D((11,)), D((11,)), D((4,)), D((4,)), D((n, 7)), D((n, 7)), D((n, 3, 2)), D((n, 3, 2))]
    scratch += [D((n, 8)), D((n, 8)), D((3, 8)), D((3, 8)), D((2 + 2 * n,))]
    anywhere = pl.BlockSpec(memory_space=pl.ANY)
    new_state, errors = pl.pallas_call(
        functools.partial(kernel, (ny, nz, rows, width, tok, CHUNKS)),
        out_shape=(jax.ShapeDtypeStruct(state.shape, bf16), jax.ShapeDtypeStruct((2,), f32)),
        in_specs=[anywhere] * 3,
        out_specs=(anywhere, pl.BlockSpec(memory_space=pltpu.SMEM)),
        scratch_shapes=scratch,
        compiler_params=pltpu.CompilerParams(
            collective_id=0, has_side_effects=True, vmem_limit_bytes=60 * 2**20
        ),
    )(state, feats, targ)
    new_state = pl.pallas_call(
        settle,
        out_shape=jax.ShapeDtypeStruct(state.shape, bf16),
        in_specs=[anywhere],
        out_specs=anywhere,
        scratch_shapes=[V(state.shape, bf16), D((8,)), D((8,))],
    )(new_state)
    return (new_state[None], errors)


def solution(mesh):
    torus = Mesh(mesh.devices.reshape(4, 8, 2, 2, mesh.shape["mp"]), AXES)
    placed = (P(BLK, None, "mp"), P(BLK, None, "mp"), P(BLK, None, "mp"))
    return jax.shard_map(
        functools.partial(on_device, (4, 8)),
        mesh=torus,
        in_specs=placed,
        out_specs=(P(BLK, None, "mp"), P()),
        check_vma=False,
    )
```

```python
import functools

import jax
import jax.numpy as jnp
from jax import lax
from jax.experimental import pallas as pl
from jax.experimental.pallas import tpu as pltpu
from jax.sharding import Mesh
from jax.sharding import PartitionSpec as P

BLK = ("blk_0", "blk_1", "blk_2", "blk_3")
AXES = ("blk_0", "blk_1", "blk_2", "blk_3", "mp")
MESH = pl.DeviceIdType.MESH
f32 = jnp.float32
bf16 = jnp.bfloat16
mix_third = 1.0 / 3.0
step_size = 0.1

CHUNKS = (32, 48, 48)
TILE = 2048
ORDER = ("F0", "J0", "H2", "P0", "F1", "J1", "U2", "C2", "I2", "O1")
EARLY = 2


def folded(value):
    rows, cols = value.shape
    total = None
    for i in range(0, rows, 8):
        for j in range(0, cols, 128):
            part = value[i : i + 8, j : j + 128]
            total = part if total is None else total + part
    return total


def kernel(dims, p_ref, h_ref, t_ref, out_ref, err_ref, *scratch):
    ny, nz, rows, width, tok, chunks = dims
    n = len(chunks)
    names = iter(scratch)
    H, TG, TT, EA, ES, ER, EZ, EY = (next(names) for _ in range(8))
    X0, X1, XH, G0, X2, ZS, ZR, RA, RB = ([next(names) for _ in range(n)] for _ in range(9))
    h_s, h_r, t_s, t_r, x_s, x_r, z_s, z_r, o_s, o_r, e_s, e_r, loc = names

    y, z = lax.axis_index("blk_0"), lax.axis_index("blk_1")
    xh, c, xl = lax.axis_index("blk_2"), lax.axis_index("blk_3"), lax.axis_index("mp")
    x = 2 * xh + xl
    b = 2 * x + c
    mine = 2 * xh + c
    k = y * nz + z
    starts = [sum(chunks[:j]) for j in range(n)]

    def ring(dx, dc):
        xd = lax.rem(x + dx, 4)
        return {"blk_2": lax.div(xd, 2), "mp": lax.rem(xd, 2), "blk_3": lax.rem(c + dc, 2)}

    def group(dk):
        kd = lax.rem(k + dk + ny * nz, ny * nz)
        return {"blk_0": lax.div(kd, nz), "blk_1": lax.rem(kd, nz)}

    def remote(src, dst, send, recv, to):
        return pltpu.make_async_remote_copy(
            src_ref=src, dst_ref=dst, send_sem=send, recv_sem=recv, device_id=to, device_id_type=MESH
        )

    offsets = [(2, 0), (2, 1), (1, 0), (3, 0), (1, 1), (3, 1), (0, 1)]
    partners = [ring(*o) for o in offsets] + [group(1), group(-1)]
    partners += [{"blk_1": lax.rem(z + d, nz)} for d in range(1, nz)]
    partners += [{"blk_0": lax.rem(y + d, ny)} for d in range(1, ny)]
    barrier = pltpu.get_barrier_semaphore()
    for to in partners:
        pl.semaphore_signal(barrier, inc=1, device_id=to, device_id_type=MESH)

    def slot(dx):
        xs = lax.rem(x + dx, 4)
        return (2 * lax.div(xs, 2) + c) * 2 + lax.rem(xs, 2)

    half = tok // 2
    first, second, whole = pl.ds(0, half), pl.ds(half, half), pl.ds(0, tok)

    def hidden_copy(i, dx, part, to, own=False):
        dst = H.at[slot(dx), part]
        return remote(h_ref.at[part] if own else dst, dst, h_s.at[i], h_r.at[i], to)

    ahead, behind, sibling = ring(1, 0), ring(3, 0), ring(0, 1)
    own_h = [
        hidden_copy(0, 0, first, ahead, True),
        hidden_copy(1, 0, second, behind, True),
        hidden_copy(2, 0, second, ahead, True),
        hidden_copy(3, 0, first, behind, True),
        hidden_copy(4, 0, whole, sibling, True),
    ]
    relay_h = [hidden_copy(5, 3, first, ahead), hidden_copy(6, 1, second, behind)]
    pass_h = [
        hidden_copy(7, 3, whole, sibling),
        hidden_copy(8, 1, whole, sibling),
        hidden_copy(9, 2, first, sibling),
        hidden_copy(10, 2, second, sibling),
    ]
    keep_h = pltpu.make_async_copy(h_ref, H.at[slot(0)], loc.at[0])

    lane = rows
    t_copies = []
    for m in range(4):
        xd, cd = 2 * xl + m // 2, m % 2
        src = t_ref.at[:, pl.ds(m * lane, lane)]
        own = jnp.logical_and(x == xd, c == cd)
        to = {"blk_2": lax.div(xd, 2), "mp": lax.rem(xd, 2), "blk_3": cd}
        t_copies.append(
            (
                own,
                remote(src, TG.at[mine], t_s.at[m], t_r.at[mine], to),
                pltpu.make_async_copy(src, TG.at[mine], loc.at[1]),
            )
        )

    def x_copies(j):
        out = []
        for i, (dx, dc) in enumerate(offsets):
            bd = 2 * lax.rem(x + dx, 4) + lax.rem(c + dc, 2)
            src = p_ref.at[pl.ds(pl.multiple_of(bd * rows + starts[j], 16), chunks[j])]
            out.append(remote(src, X0[j].at[1 + mine, xl], x_s.at[j, i], x_r.at[j, i], ring(dx, dc)))
        src = p_ref.at[pl.ds(pl.multiple_of(b * rows + starts[j], 16), chunks[j])]
        return out, pltpu.make_async_copy(src, X0[j].at[1 + mine, xl], loc.at[2 + j])

    x0 = [x_copies(j) for j in range(n)]

    def halo(j, q, direction, src, dst):
        return remote(src, dst, z_s.at[j, q, direction], z_r.at[j, q, direction], group(1 - 2 * direction))

    x0_halo = [
        (halo(j, 0, 0, X0[j].at[4], X0[j].at[0]), halo(j, 0, 1, X0[j].at[1], X0[j].at[5])) for j in range(n)
    ]
    z_halo = [
        (halo(j, 1, 0, ZS[j].at[0], ZR[j].at[1]), halo(j, 1, 1, ZS[j].at[1], ZR[j].at[0])) for j in range(n)
    ]
    x1_halo = [
        (halo(j, 2, 0, X1[j].at[3, 1], XH[j].at[1]), halo(j, 2, 1, X1[j].at[0, 0], XH[j].at[0])) for j in range(n)
    ]

    def back_copies(j):
        out = []
        for s in range(8):
            r, hf = s // 2, s % 2
            own = jnp.logical_and(x == 2 * (r // 2) + hf, c == r % 2)
            to = {"blk_2": r // 2, "mp": hf, "blk_3": r % 2}
            dst = out_ref.at[pl.ds(pl.multiple_of(b * rows + starts[j], 16), chunks[j])]
            out.append(
                (
                    own,
                    remote(X2[j].at[r, hf], dst, o_s.at[j, s], o_r.at[j, b], to),
                    pltpu.make_async_copy(X2[j].at[r, hf], dst, loc.at[2 + n + j]),
                )
            )
        return out

    back = [back_copies(j) for j in range(n)]

    def start_one(entry):
        own, away, near = entry
        pl.when(jnp.logical_not(own))(away.start)
        pl.when(own)(near.start)

    def finish_one(entry):
        own, away, near = entry
        pl.when(jnp.logical_not(own))(away.wait_send)
        pl.when(own)(near.wait)

    def forward(w_ref, base, t_start, size, out, first=0, count=4):
        def replica(i, carry):
            r = first + i

            def part(hf, acc):
                return acc + lax.dot_general(
                    w_ref[r + base, hf], H[2 * r + hf], (((1,), (1,)), ((), ())), preferred_element_type=f32
                )

            acc = lax.fori_loop(0, 2, part, jnp.zeros((size, tok), f32))
            out[r] = (acc - TT[r, pl.ds(t_start, size)]).astype(bf16)
            return carry

        lax.fori_loop(0, count, replica, 0)

    tiles = width // TILE

    def over_tiles(body, count=2):
        def step(i, carry):
            ii = lax.div(i, 2 * tiles)
            hf = lax.rem(lax.div(i, tiles), 2)
            cols = pl.ds(pl.multiple_of(lax.rem(i, tiles) * TILE, TILE), TILE)
            body(ii, hf, cols)
            return carry

        lax.fori_loop(0, 2 * count * tiles, step, 0)

    def grad(res, r, hf, cols):
        return lax.dot_general(
            res, H[2 * r + hf, :, cols], (((1,), (0,)), ((), ())), preferred_element_type=f32
        ) * (1.0 / tok)

    def update(j, r, hf, cols, where=None, g=None):
        g = grad(RA[j][r], r, hf, cols) if g is None else g
        G0[j][r, hf, :, cols] = g
        own = X0[j][r + 1, hf, :, cols].astype(f32)
        right = X0[j][r + 2, hf, :, cols].astype(f32)
        left = X0[j][r, hf, :, cols].astype(f32)
        diff = own - right
        EA[0] += folded(diff * diff)
        pull = step_size * g.astype(bf16).astype(f32)
        new = ((left + own + right) * mix_third - pull).astype(bf16)
        X1[j][r, hf, :, cols] = new
        if where is not None:
            ZS[j][where, hf, :, cols] = (new.astype(f32) - pull).astype(bf16)

    def stage_B(j):
        for copy in x0_halo[j]:
            copy.wait_recv()
        over_tiles(lambda i, hf, cols: update(j, 3 - 3 * i, hf, cols, i))
        for copy in z_halo[j] + x1_halo[j]:
            copy.start()
        over_tiles(lambda i, hf, cols: update(j, 1 + i, hf, cols))

    def pair(side):
        forward(X0[0], 1, 0, chunks[0], RA[0], 2 * side, 2)
        edge = 1 - side
        over_tiles(lambda i, hf, cols: update(0, 3 * side, hf, cols, edge), 1)
        for way in range(2):

            @pl.when(edge == way)
            def _():
                z_halo[0][way].start()
                x1_halo[0][way].start()

        over_tiles(lambda i, hf, cols: update(0, 1 + side, hf, cols), 1)

    def inner(j, i, hf, cols, g=None):
        r = 1 + i
        g = grad(RB[j][r], r, hf, cols) if g is None else g
        own = X1[j][r, hf, :, cols].astype(f32)
        right = X1[j][r + 1, hf, :, cols].astype(f32)
        left = X1[j][r - 1, hf, :, cols].astype(f32)
        diff = own - right
        EA[1] += folded(diff * diff)
        g0 = G0[j][r, hf, :, cols]
        tracks = (
            G0[j][r - 1, hf, :, cols].astype(bf16).astype(f32)
            + g0.astype(bf16).astype(f32)
            + G0[j][r + 1, hf, :, cols].astype(bf16).astype(f32)
        )
        track = (tracks * mix_third + g - g0).astype(bf16).astype(f32)
        X2[j][r, hf, :, cols] = ((left + own + right) * mix_third - step_size * track).astype(bf16)

    def outer(j, i, hf, cols, g=None):
        r, nb = 3 - 3 * i, 2 - i
        g = grad(RB[j][r], r, hf, cols) if g is None else g
        own = X1[j][r, hf, :, cols].astype(f32)
        near = X1[j][nb, hf, :, cols].astype(f32)
        far = XH[j][hf, :, cols].astype(f32)
        if j == n - 1:
            near_diff = far_diff = None
        else:
            near_diff, far_diff = own - near, own - far
        if near_diff is not None:
            near_weight = jnp.where(i == 1, 1.0, 0.0).astype(f32)
            far_weight = jnp.where(i == hf, 1.0, 0.0).astype(f32)
            EA[1] += folded(near_diff * near_diff) * near_weight + folded(far_diff * far_diff) * far_weight
        g0 = G0[j][r, hf, :, cols]
        tracks = g0.astype(bf16).astype(f32) + G0[j][nb, hf, :, cols].astype(bf16).astype(f32)
        mixed = (ZR[j][i, hf, :, cols].astype(f32) + own + near - step_size * tracks) * mix_third
        X2[j][r, hf, :, cols] = (mixed - step_size * (g - g0)).astype(bf16)

    def stage_H(j):
        for copy in x0[j][0]:
            copy.wait_recv()
        x0[j][1].wait()
        for copy in x0_halo[j]:
            copy.start()

    def stage_A(j):
        forward(X0[j], 1, starts[j], chunks[j], RA[j])

    def stage_C(j):
        forward(X1[j], 0, starts[j], chunks[j], RB[j])

    def stage_I(j):
        over_tiles(functools.partial(inner, j))
        for s in (2, 3, 4, 5):
            start_one(back[j][s])

    def stage_O(j):
        for copy in z_halo[j] + x1_halo[j]:
            copy.wait_recv()
        over_tiles(functools.partial(outer, j))

    def both(j, r, hf, cols):
        res = jnp.concatenate([RB[j][r], RA[j + 1][r]], axis=0)
        g = grad(res, r, hf, cols)
        return g[: chunks[j]], g[chunks[j] :]

    def stage_F(j):
        size = chunks[j]

        def replica(r, carry):
            def part(hf, acc):
                w = jnp.concatenate([X1[j][r, hf], X0[j + 1][r + 1, hf]], axis=0)
                return acc + lax.dot_general(w, H[2 * r + hf], (((1,), (1,)), ((), ())), preferred_element_type=f32)

            acc = lax.fori_loop(0, 2, part, jnp.zeros((size + chunks[j + 1], tok), f32))
            RB[j][r] = (acc[:size] - TT[r, pl.ds(starts[j], size)]).astype(bf16)
            RA[j + 1][r] = (acc[size:] - TT[r, pl.ds(starts[j + 1], chunks[j + 1])]).astype(bf16)
            return carry

        lax.fori_loop(0, 4, replica, 0)

    def stage_J(j):
        def body(i, hf, cols):
            g1, g0 = both(j, 1 + i, hf, cols)
            inner(j, i, hf, cols, g1)
            update(j + 1, 1 + i, hf, cols, None, g0)

        over_tiles(body)
        for s in (2, 3, 4, 5):
            start_one(back[j][s])

    def stage_P(j):
        for copy in z_halo[j] + x1_halo[j] + x0_halo[j + 1]:
            copy.wait_recv()

        def body(i, hf, cols):
            g1, g0 = both(j, 3 - 3 * i, hf, cols)
            outer(j, i, hf, cols, g1)
            update(j + 1, 3 - 3 * i, hf, cols, i, g0)

        over_tiles(body)
        for copy in z_halo[j + 1] + x1_halo[j + 1]:
            copy.start()
        send_outer(j)

    def stage_U(j):
        for copy in x0_halo[j]:
            copy.wait_recv()
        over_tiles(lambda i, hf, cols: update(j, 3 - 3 * i, hf, cols, i))
        for copy in z_halo[j] + x1_halo[j]:
            copy.start()

    def send_outer(j):
        for s in (6, 7, 0, 1):
            start_one(back[j][s])

    def issue_x0(j):
        for copy in x0[j][0]:
            copy.start()
        x0[j][1].start()

    EA[...] = jnp.zeros_like(EA)
    pl.semaphore_wait(barrier, len(partners))

    issue_x0(0)
    for copy in own_h:
        copy.start()
    keep_h.start()
    for entry in t_copies:
        start_one(entry)
    stage_H(0)
    own_h[0].wait_recv()
    for j in range(1, EARLY):
        issue_x0(j)
    relay_h[0].start()
    own_h[1].wait_recv()
    relay_h[1].start()
    for j in range(EARLY, n):
        issue_x0(j)
    for r in range(4):
        own = jnp.logical_and(r == mine, xl == xh)
        arrival = remote(TG.at[r], TG.at[r], t_s.at[0], t_r.at[r], sibling)
        pl.when(jnp.logical_not(own))(arrival.wait_recv)
    for entry in t_copies:
        finish_one(entry)

    def turn(r, carry):
        TT[r] = TG[r].astype(f32).T
        return carry

    lax.fori_loop(0, 4, turn, 0)
    own_h[2].wait_recv()
    pass_h[0].start()
    own_h[3].wait_recv()
    pass_h[1].start()
    own_h[4].wait_recv()
    keep_h.wait()
    pass_h[0].wait_recv()
    pass_h[1].wait_recv()
    for copy in x0_halo[0]:
        copy.wait_recv()
    pair(xh)
    for j in range(1, EARLY):
        stage_H(j)
    relay_h[0].wait_recv()
    pass_h[2].start()
    relay_h[1].wait_recv()
    pass_h[3].start()
    pass_h[2].wait_recv()
    pass_h[3].wait_recv()
    pair(1 - xh)

    stages = {"F": stage_F, "J": stage_J, "P": stage_P, "U": stage_U}
    stages |= {"H": stage_H, "A": stage_A, "B": stage_B, "C": stage_C, "I": stage_I, "O": stage_O}
    for step in ORDER:
        stages[step[0]](int(step[1]))
        if step[0] == "O":
            send_outer(int(step[1]))
    last = n - 1
    for copy in z_halo[last] + x1_halo[last]:
        copy.wait_recv()

    def last_edges(i, carry):
        hf = lax.div(i, tiles)
        cols = pl.ds(pl.multiple_of(lax.rem(i, tiles) * TILE, TILE), TILE)
        near = X1[last][0, hf, :, cols].astype(f32) - X1[last][1, hf, :, cols].astype(f32)
        far = X1[last][3 - 3 * hf, hf, :, cols].astype(f32) - XH[last][hf, :, cols].astype(f32)
        EA[1] += folded(near * near) + folded(far * far)
        return carry

    lax.fori_loop(0, 2 * tiles, last_edges, 0)
    sums = [jnp.sum(EA[i], axis=0, keepdims=True) for i in range(2)]
    row = lax.broadcasted_iota(jnp.int32, (8, 128), 0)
    ES[0] = jnp.where(row == 0, sums[0], jnp.where(row == 1, sums[1], 0.0))
    ER[b] = ES[0]
    e0 = []
    for i, (dx, dc) in enumerate(offsets):
        copy = remote(ES.at[0], ER.at[b], e_s.at[0, i], e_r.at[0, i], ring(dx, dc))
        copy.start()
        e0.append(copy)
    over_tiles(functools.partial(outer, last))
    send_outer(last)
    for copy in e0:
        copy.wait_recv()
    total = ER[0]
    for i in range(1, 8):
        total = total + ER[i]
    ES[1] = total
    EZ[z] = total
    e1 = []
    for d in range(1, nz):
        copy = remote(ES.at[1], EZ.at[z], e_s.at[1, d], e_r.at[1, d], {"blk_1": lax.rem(z + d, nz)})
        copy.start()
        e1.append(copy)
    for copy in e1:
        copy.wait_recv()
    total = EZ[0]
    for i in range(1, nz):
        total = total + EZ[i]
    ES[2] = total
    EY[y] = total
    e2 = []
    for d in range(1, ny):
        copy = remote(ES.at[2], EY.at[y], e_s.at[2, d], e_r.at[2, d], {"blk_0": lax.rem(y + d, ny)})
        copy.start()
        e2.append(copy)
    for copy in e2:
        copy.wait_recv()
    total = EY[0]
    for i in range(1, ny):
        total = total + EY[i]
    for i in range(2):
        err_ref[i] = jnp.sum(total[i : i + 1]) / (2 * width * 4 * ny * nz)

    for j in range(n):
        for s in range(8):
            arrival = remote(X2[j].at[0, 0], out_ref.at[pl.ds(starts[j], chunks[j])], o_s.at[j, 0], o_r.at[j, s], sibling)
            pl.when(s != b)(arrival.wait_recv)
    for copy in own_h + relay_h + pass_h + e0 + e1 + e2:
        copy.wait_send()
    for j in range(n):
        for copy in list(x0[j][0]) + list(x0_halo[j] + z_halo[j] + x1_halo[j]):
            copy.wait_send()
        for entry in back[j]:
            finish_one(entry)


def settle(src, dst, hold, s_in, s_out):
    parts = 8
    size = src.shape[0] // parts
    loads = [
        pltpu.make_async_copy(src.at[pl.ds(i * size, size)], hold.at[pl.ds(i * size, size)], s_in.at[i])
        for i in range(parts)
    ]
    stores = [
        pltpu.make_async_copy(hold.at[pl.ds(i * size, size)], dst.at[pl.ds(i * size, size)], s_out.at[i])
        for i in range(parts)
    ]
    for load in loads:
        load.start()
    for load, store in zip(loads, stores):
        load.wait()
        store.start()
    for store in stores:
        store.wait()


def on_device(sizes, params, hidden, targets):
    ny, nz = sizes
    state, feats, targ = params[0], hidden[0], targets[0]
    depth, width = state.shape
    tok = feats.shape[0]
    rows = depth // 8
    n = len(CHUNKS)
    V, D = pltpu.VMEM, pltpu.SemaphoreType.DMA
    scratch = [
        V((8, tok, width), bf16),
        V((4, tok, rows), bf16),
        V((4, rows, tok), f32),
        V((2, 8, 128), f32),
        V((3, 8, 128), f32),
        V((8, 8, 128), f32),
        V((nz, 8, 128), f32),
        V((ny, 8, 128), f32),
    ]
    scratch += [V((6, 2, r, width), bf16) for r in CHUNKS]
    scratch += [V((4, 2, r, width), bf16) for r in CHUNKS]
    scratch += [V((2, r, width), bf16) for r in CHUNKS]
    scratch += [V((4, 2, r, width), f32) for r in CHUNKS]
    scratch += [V((4, 2, r, width), bf16) for r in CHUNKS]
    scratch += [V((2, 2, r, width), bf16) for r in CHUNKS]
    scratch += [V((2, 2, r, width), bf16) for r in CHUNKS]
    scratch += [V((4, r, tok), bf16) for r in CHUNKS]
    scratch += [V((4, r, tok), bf16) for r in CHUNKS]
    scratch += [D((11,)), D((11,)), D((4,)), D((4,)), D((n, 7)), D((n, 7)), D((n, 3, 2)), D((n, 3, 2))]
    scratch += [D((n, 8)), D((n, 8)), D((3, 8)), D((3, 8)), D((2 + 2 * n,))]
    anywhere = pl.BlockSpec(memory_space=pl.ANY)
    new_state, errors = pl.pallas_call(
        functools.partial(kernel, (ny, nz, rows, width, tok, CHUNKS)),
        out_shape=(jax.ShapeDtypeStruct(state.shape, bf16), jax.ShapeDtypeStruct((2,), f32)),
        in_specs=[anywhere] * 3,
        out_specs=(anywhere, pl.BlockSpec(memory_space=pltpu.SMEM)),
        scratch_shapes=scratch,
        compiler_params=pltpu.CompilerParams(
            collective_id=0, has_side_effects=True, vmem_limit_bytes=60 * 2**20
        ),
    )(state, feats, targ)
    new_state = pl.pallas_call(
        settle,
        out_shape=jax.ShapeDtypeStruct(state.shape, bf16),
        in_specs=[anywhere],
        out_specs=anywhere,
        scratch_shapes=[V(state.shape, bf16), D((8,)), D((8,))],
    )(new_state)
    return (new_state[None], errors)


def solution(mesh):
    torus = Mesh(mesh.devices.reshape(4, 8, 2, 2, mesh.shape["mp"]), AXES)
    placed = (P(BLK, None, "mp"), P(BLK, None, "mp"), P(BLK, None, "mp"))
    return jax.shard_map(
        functools.partial(on_device, (4, 8)),
        mesh=torus,
        in_specs=placed,
        out_specs=(P(BLK, None, "mp"), P()),
        check_vma=False,
    )
```
